32 devices in a mesh: row: 4 (over y, core), col: 8 (over z, x).
Axes of the slice: x: 2, y: 2, z: 4, core: 2. Of those that a mesh axis runs over, the one named last changes fastest.
Arguments:
- hidden_acts: bfloat16 [256, 29568], P('row', 'col'), may hold values from -6 to 6
- output_errors: bfloat16 [256, 4096], P('col', 'row'), may hold values from -6 to 6
- col_points: int32 [8], replicated, may hold values from 0 to 16, as said below
- row_points: int32 [4], replicated, may hold values from 0 to 8, as said below
- worker_mask: int32 [4, 8], replicated, may hold values from 0 to 1, as said below
Outputs:
- clipped_grad: float32 [2, 2048, 29568], P(None, 'col', 'row')
The draws below stay inside these ranges and needn't reach their ends.
Inputs may be any that keep to these rules, and one draw needn't show every extreme that they name: `col_points`: distinct node indices. `row_points`: distinct node indices. `worker_mask`: each row of the grid has between 1 and 2 erased workers.
All inputs are finite; a program needn't handle non-finite values.
Results may differ from the reference program's by a relative error of at most 0.02.
Values may be sent and summed in bfloat16 or wider, within the bound.
A program may use at most 192 MiB of HBM per device.

```python
import jax
import jax.numpy as jnp
from jax import lax

D = 4096
FF = 29568
TOKENS = 256
N_ROW = 4
N_COL = 8


def draw_col_points(key, part):
    return jax.random.permutation(key, 2 * N_COL + 1)[:N_COL].astype(jnp.int32)


def draw_row_points(key, part):
    return jax.random.permutation(key, 2 * N_ROW + 1)[:N_ROW].astype(jnp.int32)


def one_order(row_key):
    return jax.random.permutation(row_key, N_COL)


def draw_worker_mask(key, part):
    key_count = jax.random.fold_in(key, 11)
    key_order = jax.random.fold_in(key, 23)
    counts = jax.random.randint(key_count, (N_ROW,), 1, N_COL // 4 + 1)
    counts = jnp.where(jnp.arange(N_ROW) == 0, N_COL // 4, counts)
    orders = jax.vmap(one_order)(jax.random.split(key_order, N_ROW))
    return jnp.where(orders < counts[:, None], 0, 1).astype(jnp.int32)


def shard_levels(own_key, extent, cuts, smallest, high):
    level, own = 1.0, jax.random.fold_in(own_key, 6)
    for dim, parts in cuts:
        draws = jnp.exp(jax.random.uniform(jax.random.fold_in(own, dim), (parts,), jnp.float32, smallest / len(cuts), high / len(cuts)))
        level = level * jnp.repeat(draws, extent[dim] // parts).reshape([-1 if axis == dim else 1 for axis in range(len(extent))])
    return level


def noise(own_key, shape, spread, reach, cuts=(), dtype=jnp.bfloat16):
    factor_of = shard_levels(own_key, shape, cuts, -0.22, 0.18) if cuts else 1.0
    values = jax.random.normal(own_key, shape, jnp.float32) * spread * factor_of
    return jnp.minimum(jnp.maximum(values, -reach), reach).astype(dtype)


def setup_inputs(seed: int = 0) -> dict:
    key_list = jax.random.split(jax.random.key(seed), 6)
    return {
        "hidden_acts": noise(key_list[0], (TOKENS, FF), 1.0, 6.0, ((0, 4), (1, 8))),
        "output_errors": noise(key_list[1], (TOKENS, D), 1.0, 6.0, ((0, 8), (1, 4))),
        "col_points": draw_col_points(jax.random.fold_in(key_list[5], 71), 0),
        "row_points": draw_row_points(jax.random.fold_in(key_list[5], 71), 0),
        "worker_mask": draw_worker_mask(jax.random.fold_in(key_list[5], 71), 0),
    }


def node_value(index, count):
    return jnp.cos(jnp.pi * (2.0 * index.astype(jnp.float32) + 1.0) / (2.0 * count))

def berrut(nodes, signs, live, targets):
    terms = (live * signs)[:, None] / (targets[None, :] - nodes[:, None])
    return terms / lax.optimization_barrier(jnp.sum(terms, axis=0, keepdims=True))

def rank_signs(points, live):
    lower = (points[None, :] < points[:, None]).astype(jnp.int32)
    ranks = lax.optimization_barrier(jnp.sum(lower * live[None, :], axis=1))
    return (1 - 2 * (ranks % 2)).astype(jnp.float32)

def reference(hidden_acts, output_errors, col_points, row_points, worker_mask):
    act_blocks = N_COL // 2
    err_blocks = N_ROW // 2
    act_width = FF // act_blocks
    err_width = D // err_blocks
    data_acts = node_value(jnp.arange(act_blocks), act_blocks)
    data_errs = node_value(jnp.arange(err_blocks), err_blocks)
    work_acts = node_value(col_points, 2 * N_COL + 1)
    work_errs = node_value(row_points, 2 * N_ROW + 1)
    alt_acts = (1 - 2 * (jnp.arange(act_blocks) % 2)).astype(jnp.float32)
    alt_errs = (1 - 2 * (jnp.arange(err_blocks) % 2)).astype(jnp.float32)
    encode_acts = berrut(data_acts, alt_acts, jnp.ones((act_blocks,), jnp.float32), work_acts)
    encode_errs = berrut(data_errs, alt_errs, jnp.ones((err_blocks,), jnp.float32), work_errs)
    blocks_acts = hidden_acts.astype(jnp.float32).reshape(TOKENS, act_blocks, act_width)
    coded_acts = jnp.einsum('kj,tkf->jtf', encode_acts, blocks_acts).astype(jnp.bfloat16)
    blocks_errs = output_errors.astype(jnp.float32).reshape(TOKENS, err_blocks, err_width)
    coded_errs = jnp.einsum('li,tld->itd', encode_errs, blocks_errs).astype(jnp.bfloat16)
    all_rows = jnp.ones((N_ROW,), jnp.int32)
    decode_errs = berrut(work_errs, rank_signs(row_points, all_rows), jnp.ones((N_ROW,), jnp.float32), data_errs)
    acts_wide = coded_acts.astype(jnp.float32)

    def one_row(total, index):
        errs_here = coded_errs[index].astype(jnp.float32)
        product = jnp.einsum('td,jtf->jdf', errs_here, acts_wide).astype(jnp.bfloat16)
        live = worker_mask[index]
        decode_acts = berrut(work_acts, rank_signs(col_points, live), live.astype(jnp.float32), data_acts)
        decoded = jnp.einsum('jk,jdf->dkf', decode_acts, product.astype(jnp.float32))
        decoded = decoded.reshape(err_width, FF).astype(jnp.bfloat16)
        total = total + decode_errs[index][:, None, None] * decoded.astype(jnp.float32)[None]
        return (total, None)
    start = jnp.zeros((err_blocks, err_width, FF), jnp.float32)
    grad, unused = lax.scan(one_row, start, jnp.arange(N_ROW))
    squares = jnp.sum(grad * grad)
    factor = jnp.minimum(1.0, jnp.sqrt(jnp.float32(FF * D)) / jnp.sqrt(squares + 1e-06))
    return grad * factor
```

```python
import functools

import jax
import jax.numpy as jnp
from jax import lax
from jax.experimental import pallas as pl
from jax.experimental.pallas import tpu as pltpu
from jax.sharding import PartitionSpec as P

LANES = 128


def node_value(index, count):
    return jnp.cos(jnp.pi * (2.0 * index.astype(jnp.float32) + 1.0) / (2.0 * count))


def berrut(nodes, signs, live, targets):
    terms = (live * signs)[..., :, None] / (targets[None, :] - nodes[:, None])
    return terms / jnp.sum(terms, axis=-2, keepdims=True)


def rank_signs(points, live):
    lower = (points[None, :] < points[:, None]).astype(jnp.int32)
    ranks = jnp.sum(lower * live[..., None, :], axis=-1)
    return (1 - 2 * (ranks % 2)).astype(jnp.float32)


def mixing(col_points, row_points, worker_mask, act_blocks, err_blocks, block):
    row_count, col_count = worker_mask.shape
    data_acts = node_value(jnp.arange(act_blocks), act_blocks)
    data_errs = node_value(jnp.arange(err_blocks), err_blocks)
    work_acts = node_value(col_points, 2 * col_count + 1)
    work_errs = node_value(row_points, 2 * row_count + 1)
    alt_acts = (1 - 2 * (jnp.arange(act_blocks) % 2)).astype(jnp.float32)
    alt_errs = (1 - 2 * (jnp.arange(err_blocks) % 2)).astype(jnp.float32)
    encode_acts = berrut(data_acts, alt_acts, jnp.ones((act_blocks,), jnp.float32), work_acts)
    encode_errs = berrut(data_errs, alt_errs, jnp.ones((err_blocks,), jnp.float32), work_errs)
    all_rows = jnp.ones((row_count,), jnp.int32)
    decode_errs = berrut(
        work_errs, rank_signs(row_points, all_rows), all_rows.astype(jnp.float32), data_errs
    )
    target = lax.dynamic_slice_in_dim(data_acts, block, 1, 0)
    decode_acts = berrut(
        work_acts, rank_signs(col_points, worker_mask), worker_mask.astype(jnp.float32), target
    )[..., 0]
    through = jnp.sum(decode_acts[:, None, :] * encode_acts[None], axis=-1)
    return jnp.sum(
        decode_errs.T[:, None, None, :] * encode_errs[None, :, None, :] * through.T[None, None],
        axis=-1,
    )


def place_in_tiles(piece, part, parts, chunk):
    width = piece.shape[1]
    placed = None
    for index in range(parts):
        shift = index * width % LANES
        here = jnp.pad(piece, ((0, 0), (shift, chunk - shift - width)))
        placed = here if placed is None else jnp.where(part == index, here, placed)
    return placed


def product_kernel(bases, step, mix_ref, acts_ref, grad_ref, square_ref):
    part, tile = pl.program_id(0), pl.program_id(1)
    lead, groups, width = grad_ref.shape
    rows = lead * groups
    depth = acts_ref.shape[0] * acts_ref.shape[1]
    result = jnp.dot(
        mix_ref[...], acts_ref[...].reshape(depth, step), preferred_element_type=jnp.float32
    )
    for index, base in enumerate(bases):
        for turn in range(pl.num_programs(1)):
            start = base + turn * step

            @pl.when((part == index) & (tile == turn))
            def _():
                size = min(step, width - start)
                shared = LANES if index > 0 and turn == 0 else 0
                for block in range(lead):
                    here = result[block * groups : (block + 1) * groups]
                    if shared:
                        grad_ref[block, :, start : start + shared] += here[:, :shared]
                    grad_ref[block, :, start + shared : start + size] = here[:, shared:size]

    @pl.when((part == len(bases) - 1) & (tile == pl.num_programs(1) - 1))
    def _():
        strip = 8

        def add(index, total):
            for block in range(lead):
                piece = grad_ref[block, pl.ds(pl.multiple_of(index * strip, strip), strip), :]
                total = total + piece * piece
            return total

        total = lax.fori_loop(0, groups // strip, add, jnp.zeros((strip, width), jnp.float32))
        square_ref[0, 0] = jnp.sum(total)


def scale_kernel(factor_ref, grad_ref, out_ref, stage, sem):
    lead, groups, width = grad_ref.shape
    strip = stage.shape[1]
    count = lead * groups // strip
    per = groups // strip

    def copy(index, slot):
        return pltpu.make_async_copy(
            stage.at[slot],
            out_ref.at[index // per, pl.ds(pl.multiple_of(index % per * strip, strip), strip), :],
            sem.at[slot],
        )

    @pl.loop(0, count)
    def _(index):
        slot = index % 4

        @pl.when(index >= 4)
        def _():
            copy(index - 4, slot).wait()

        stage[slot] = (
            grad_ref[index // per, pl.ds(pl.multiple_of(index % per * strip, strip), strip), :]
            * factor_ref[0]
        )
        copy(index, slot).start()

    for index in range(count - 4, count):
        copy(index, index % 4).wait()


def solution(mesh):
    row_count, col_count = mesh.shape["row"], mesh.shape["col"]
    act_blocks, err_blocks = col_count // 2, row_count // 2
    parts = col_count // act_blocks
    assert act_blocks == row_count

    def shards(hidden_acts, output_errors, col_points, row_points, worker_mask):
        row_place, col_place = lax.axis_index("row"), lax.axis_index("col")
        width = hidden_acts.shape[1]
        tokens = hidden_acts.shape[0] * row_count
        act_width = width * parts
        bases = [part * width // LANES * LANES for part in range(parts)]
        chunk = max(
            -(-((part + 1) * width - base) // LANES) * LANES for part, base in enumerate(bases)
        )
        groups = output_errors.shape[1] * row_count // err_blocks // col_count
        acts = lax.all_gather(
            place_in_tiles(hidden_acts, col_place % parts, parts, chunk),
            ("col", "row"),
            axis=0,
            tiled=True,
        ).reshape(act_blocks, parts, tokens, chunk)

        errs = lax.all_gather(output_errors, "row", axis=1, tiled=True)
        errs = errs.reshape(errs.shape[0], err_blocks, col_count, groups)
        errs = lax.all_to_all(errs, "col", split_axis=2, concat_axis=0, tiled=True)[:, :, 0]
        mix = mixing(col_points, row_points, worker_mask, act_blocks, err_blocks, row_place)
        source = errs.astype(jnp.float32)
        left = sum(
            mix[:, m, :, None, None] * source[:, m].T[None, None] for m in range(err_blocks)
        )
        left = left.astype(jnp.bfloat16)
        left = left.transpose(0, 2, 1, 3).reshape(err_blocks * groups, act_blocks * tokens)

        tiles = chunk // LANES
        step = LANES * max(n for n in range(1, 7) if tiles % n == 0)
        shape = (err_blocks, groups, act_width)
        grad, squares = pl.pallas_call(
            functools.partial(product_kernel, bases, step),
            grid=(parts, chunk // step),
            in_specs=[
                pl.BlockSpec(left.shape, lambda part, tile: (0, 0)),
                pl.BlockSpec(
                    (act_blocks, None, tokens, step), lambda part, tile: (0, part, 0, tile)
                ),
            ],
            out_specs=[
                pl.BlockSpec(memory_space=pltpu.VMEM),
                pl.BlockSpec(memory_space=pltpu.SMEM),
            ],
            out_shape=[
                pltpu.VMEM(shape, jnp.float32),
                jax.ShapeDtypeStruct((1, 1), jnp.float32),
            ],
            compiler_params=pltpu.CompilerParams(vmem_limit_bytes=40 * 2**20),
            cost_estimate=pl.CostEstimate(
                flops=4 * left.size * act_width,
                bytes_accessed=acts.size * 2,
                transcendentals=0,
            ),
            name="product",
        )(left, acts)
        squares = lax.psum(squares[0, 0], ("row", "col"))
        size = shape[0] * shape[1] * shape[2] * row_count * col_count
        factor = jnp.minimum(1.0, jnp.sqrt(jnp.float32(size)) / jnp.sqrt(squares + 1e-06))
        strip = min(32, groups)
        return pl.pallas_call(
            scale_kernel,
            in_specs=[
                pl.BlockSpec(memory_space=pltpu.SMEM),
                pl.BlockSpec(memory_space=pltpu.VMEM),
            ],
            out_specs=pl.BlockSpec(memory_space=pl.ANY),
            out_shape=jax.ShapeDtypeStruct(shape, jnp.float32),
            scratch_shapes=[
                pltpu.VMEM((4, strip, act_width), jnp.float32),
                pltpu.SemaphoreType.DMA((4,)),
            ],
            compiler_params=pltpu.CompilerParams(vmem_limit_bytes=40 * 2**20),
            name="scale",
        )(factor[None], grad)

    return jax.shard_map(
        shards,
        mesh=mesh,
        in_specs=(P("row", "col"), P("col", "row"), P(), P(), P()),
        out_specs=P(None, "col", "row"),
        check_vma=False,
    )
```
